768 devices in a mesh: rep: 4 (over y_lo, core), row: 16 (over y_hi, x), col: 12 (over z).
Axes of the slice: x: 4, y: 8 (y_hi: 4, y_lo: 2; y = y_hi * 2 + y_lo), z: 12, core: 2. Of those that a mesh axis runs over, the one named last changes fastest.
Arguments:
- delta: bfloat16 [4, 8192, 4608], P('rep', 'row', 'col'), may hold values from -6 to 6
- params: float32 [8192, 4608], P('row', 'col'), may hold values from -6 to 6
- momentum: float32 [8192, 4608], P('row', 'col'), may hold values from -3 to 3
Outputs:
- params_next: float32 [8192, 4608], P('row', 'col')
- momentum_next: float32 [8192, 4608], P('row', 'col')
- weights: bfloat16 [8192, 4608], P(None, 'col')
The draws below stay inside these ranges and needn't reach their ends.
All inputs are finite; a program needn't handle non-finite values.
Results may differ from the reference program's by a relative error of at most 0.0075.
Values may be sent and summed in bfloat16 or wider, within the bound.
No kernel may reach another device: no remote copies, remote signals or barrier semaphores. Data moves between devices by JAX's collectives and lax.ppermute only.
A program may use at most 64 MiB of HBM per device.

```python
import jax
import jax.numpy as jnp

D = 8192
COLS = 4608
REPS = 4


def steps_of(stream_key, extent, cuts, smallest, largest):
    loudness, own = 1.0, jax.random.fold_in(stream_key, 6)
    for dim, parts in cuts:
        steps = jnp.exp(jax.random.uniform(jax.random.fold_in(own, dim), (parts,), jnp.float32, smallest / len(cuts), largest / len(cuts)))
        loudness = loudness * jnp.repeat(steps, extent[dim] // parts).reshape([-1 if axis == dim else 1 for axis in range(len(extent))])
    return loudness


def gaussian(stream_key, dims, scale, limit, shards=(), held_as=jnp.bfloat16):
    result = scale * jax.random.normal(stream_key, dims, jnp.float32)
    if shards:
        result = result * steps_of(stream_key, dims, shards, -0.22, 0.18)
    return jnp.clip(result, -limit, limit).astype(held_as)


def setup_inputs(seed: int = 0) -> dict:
    key_of = jax.random.split(jax.random.key(seed), 4)
    delta = gaussian(key_of[0], (REPS, D, COLS), 1.0, 6.0, ((0, 4), (1, 16), (2, 12)))
    params = gaussian(key_of[1], (D, COLS), 1.0, 6.0, ((0, 16), (1, 12)), jnp.float32)
    momentum = gaussian(key_of[2], (D, COLS), 0.5, 3.0, ((0, 16), (1, 12)), jnp.float32)
    return dict(delta=delta, params=params, momentum=momentum)


def reference(delta, params, momentum):
    total = jnp.sum(delta.astype(jnp.float32), axis=0)
    average = total / delta.shape[0]
    momentum_next = 0.9 * momentum + average
    params_next = params - 0.7 * (average + 0.9 * momentum_next)
    weights = params_next.astype(jnp.bfloat16)
    return params_next, momentum_next, weights
```

```python
import jax
import jax.numpy as jnp
from jax import lax
from jax.experimental import pallas as pl
from jax.experimental.pallas import tpu as pltpu
from jax.sharding import PartitionSpec as P

PLANE = ("rep", "row")
NX, NY = 4, 8


def index(x, y, core):
    return ((y % NY % 2) * 2 + core) * (NX * NY // 2) + (y % NY // 2) * NX + x % NX


def beside(i, core):
    return i + 1 - 2 * ((i + core) % 2)


def send(array, partner):
    pairs = [
        (index(x, y, core), index(*partner(x, y, core)))
        for x in range(NX)
        for y in range(NY)
        for core in range(2)
    ]
    return lax.ppermute(array, PLANE, pairs)


def far_groups():
    return [
        [index(x + 2 * j, y + 2 * i, core) for i in range(NY // 2) for j in range(NX // 2)]
        for x in range(2)
        for y in range(2)
        for core in range(2)
    ]


def update(average, params, momentum):
    momentum_next = 0.9 * momentum + average
    params_next = params - 0.7 * (average + 0.9 * momentum_next)
    return (params_next, momentum_next)


def quarter_kernel(parts_ref, params_ref, momentum_ref, average_ref, weights_ref):
    reps, rows, _ = parts_ref.shape
    at = pl.ds(pl.multiple_of(lax.axis_index("rep") * rows, rows), rows)
    total = parts_ref[0].astype(jnp.float32)
    for i in range(1, reps):
        total += parts_ref[i].astype(jnp.float32)
    average = total / reps
    average_ref[...] = average
    params_next, _ = update(average, params_ref[at], momentum_ref[at])
    for i in range(weights_ref.shape[0]):
        weights_ref[i] = params_next.astype(jnp.bfloat16)


def whole_kernel(own_ref, y_ref, core_ref, both_ref, params_ref, momentum_ref, params_out, momentum_out):
    rep = lax.axis_index("rep")
    y, core = rep // 2, lax.rem(rep, 2)
    rows = own_ref.shape[0]
    for ref, flip_y, flip_core in ((own_ref, 0, 0), (y_ref, 1, 0), (core_ref, 0, 1), (both_ref, 1, 1)):
        block = (1 - y if flip_y else y) * 2 + (1 - core if flip_core else core)
        at = pl.ds(pl.multiple_of(block * rows, rows), rows)
        params_out[at], momentum_out[at] = update(ref[...], params_ref[at], momentum_ref[at])


def place_kernel(flips, n, *refs):
    out_ref, sems = refs[-2:]
    rep, row = lax.axis_index("rep"), lax.axis_index("row")
    x, y, core = lax.rem(row, 2), rep // 2, lax.rem(rep, 2)
    copies = []
    for i, (ref, (fx, fy, fc)) in enumerate(zip(refs[:n], flips)):
        far, rows, _ = ref.shape
        near = ((1 - x if fx else x) * 2 + (1 - y if fy else y)) * 2 + (1 - core if fc else core)
        for k in range(far):
            at = pl.multiple_of((k * 8 + near) * rows, rows)
            copy = pltpu.make_async_copy(ref.at[k], out_ref.at[pl.ds(at, rows)], sems.at[i, k])
            copy.start()
            copies.append(copy)
    for copy in copies:
        copy.wait()


def place(blocks, out, shape):
    arrays, flips = zip(*blocks)
    n = len(arrays)
    far = arrays[0].shape[0]
    kernel = lambda *refs: place_kernel(flips, n, *refs)
    operands = arrays if out is None else (*arrays, out)
    return pl.pallas_call(
        kernel,
        name="place",
        out_shape=jax.ShapeDtypeStruct(shape, jnp.bfloat16),
        in_specs=[pl.BlockSpec(memory_space=pl.ANY)] * len(operands),
        out_specs=pl.BlockSpec(memory_space=pl.ANY),
        scratch_shapes=[pltpu.SemaphoreType.DMA((n, far))],
        input_output_aliases={} if out is None else {n: 0},
        compiler_params=pltpu.CompilerParams(vmem_limit_bytes=1 << 20),
        cost_estimate=pl.CostEstimate(
            flops=n * 1000000, bytes_accessed=2 * 2 * n * arrays[0].size, transcendentals=0
        ),
    )(*operands)


VMEM = pl.BlockSpec(memory_space=pltpu.VMEM)


def on_device(delta, params, momentum):
    reps = lax.axis_size("rep")
    rows, columns = params.shape[0] // reps, params.shape[1]
    groups = far_groups()
    block = jax.ShapeDtypeStruct((rows, columns), jnp.float32)
    whole = jax.ShapeDtypeStruct(params.shape, jnp.float32)
    small = pltpu.CompilerParams(vmem_limit_bytes=8 << 20)

    parts = lax.all_to_all(delta[0].reshape(reps, rows, columns), "rep", 0, 0, tiled=True)
    average, weights = pl.pallas_call(
        quarter_kernel,
        name="quarter",
        out_shape=(block, jax.ShapeDtypeStruct((len(groups[0]), rows, columns), jnp.bfloat16)),
        in_specs=[VMEM] * 3,
        out_specs=(VMEM, VMEM),
        compiler_params=small,
    )(parts, params, momentum)

    own = lax.all_to_all(weights, PLANE, 0, 0, axis_index_groups=groups, tiled=True)
    by_x = send(own, lambda x, y, core: (beside(x, core), y, core))
    by_y = send(own, lambda x, y, core: (x, beside(y, core), core))
    by_both = send(own, lambda x, y, core: (beside(x, core), beside(y, core), core))
    other_core = lambda x, y, core: (x, y, 1 - core)
    shape = (params.shape[0] * NX * NY // 2, columns)
    out = place(
        [(own, (0, 0, 0)), (send(own, other_core), (0, 0, 1)), (by_x, (1, 0, 0)), (by_y, (0, 1, 0))],
        None,
        shape,
    )
    out = place(
        [
            (send(by_x, other_core), (1, 0, 1)),
            (send(by_y, other_core), (0, 1, 1)),
            (by_both, (1, 1, 0)),
            (send(by_both, other_core), (1, 1, 1)),
        ],
        out,
        shape,
    )

    average_y = send(average, lambda x, y, core: (x, y ^ 1, core))
    params_next, momentum_next = pl.pallas_call(
        whole_kernel,
        name="whole",
        out_shape=(whole, whole),
        in_specs=[VMEM] * 6,
        out_specs=(VMEM, VMEM),
        compiler_params=small,
        cost_estimate=pl.CostEstimate(flops=1000000, bytes_accessed=5 << 20, transcendentals=0),
    )(average, average_y, send(average, other_core), send(average_y, other_core), params, momentum)
    return (params_next, momentum_next, out)


def solution(mesh):
    return jax.shard_map(
        on_device,
        mesh=mesh,
        in_specs=(P("rep", "row", "col"), P("row", "col"), P("row", "col")),
        out_specs=(P("row", "col"), P("row", "col"), P(None, "col")),
        check_vma=False,
    )
```

```python
import jax
import jax.numpy as jnp
from jax import lax
from jax.experimental import pallas as pl
from jax.experimental.pallas import tpu as pltpu
from jax.sharding import PartitionSpec as P


PLANE = ("rep", "row")
NX, NY = 4, 8


def index(x, y, core):
    return ((y % NY % 2) * 2 + core) * (NX * NY // 2) + (y % NY // 2) * NX + x % NX


def beside(i, core):
    return i + 1 - 2 * ((i + core) % 2)


def send(array, partner):
    pairs = [
        (index(x, y, core), index(*partner(x, y, core)))
        for x in range(NX)
        for y in range(NY)
        for core in range(2)
    ]
    return lax.ppermute(array, PLANE, pairs)


def far_groups():
    return [
        [index(x + 2 * j, y + 2 * i, core) for i in range(NY // 2) for j in range(NX // 2)]
        for x in range(2)
        for y in range(2)
        for core in range(2)
    ]


def update(average, params, momentum):
    momentum_next = 0.9 * momentum + average
    params_next = params - 0.7 * (average + 0.9 * momentum_next)
    return (params_next, momentum_next)


def quarter_kernel(parts_ref, params_ref, momentum_ref, average_ref, weights_ref):
    reps = parts_ref.shape[0]
    total = parts_ref[0].astype(jnp.float32)
    for i in range(1, reps):
        total += parts_ref[i].astype(jnp.float32)
    average = total / reps
    average_ref[...] = average
    params_next, _ = update(average, params_ref[...], momentum_ref[...])
    for i in range(weights_ref.shape[0]):
        weights_ref[i] = params_next.astype(jnp.bfloat16)


def whole_kernel(own_ref, y_ref, core_ref, both_ref, params_ref, momentum_ref, params_out, momentum_out):
    rep = lax.axis_index("rep")
    y, core = rep // 2, lax.rem(rep, 2)
    rows = own_ref.shape[0]
    for ref, flip_y, flip_core in ((own_ref, 0, 0), (y_ref, 1, 0), (core_ref, 0, 1), (both_ref, 1, 1)):
        block = (1 - y if flip_y else y) * 2 + (1 - core if flip_core else core)
        at = pl.ds(pl.multiple_of(block * rows, rows), rows)
        params_out[at], momentum_out[at] = update(ref[...], params_ref[at], momentum_ref[at])


def place_kernel(flips, n, *refs):
    out_ref, sems = refs[-2:]
    rep, row = lax.axis_index("rep"), lax.axis_index("row")
    x, y, core = lax.rem(row, 2), rep // 2, lax.rem(rep, 2)
    copies = []
    for i, (ref, (fx, fy, fc)) in enumerate(zip(refs[:n], flips)):
        far, rows, _ = ref.shape
        near = ((1 - x if fx else x) * 2 + (1 - y if fy else y)) * 2 + (1 - core if fc else core)
        for k in range(far):
            at = pl.multiple_of((k * 8 + near) * rows, rows)
            copy = pltpu.make_async_copy(ref.at[k], out_ref.at[pl.ds(at, rows)], sems.at[i, k])
            copy.start()
            copies.append(copy)
    for copy in copies:
        copy.wait()


def place(blocks, out, shape):
    arrays, flips = zip(*blocks)
    n = len(arrays)
    far = arrays[0].shape[0]
    kernel = lambda *refs: place_kernel(flips, n, *refs)
    operands = arrays if out is None else (*arrays, out)
    return pl.pallas_call(
        kernel,
        name="place",
        out_shape=jax.ShapeDtypeStruct(shape, jnp.bfloat16),
        in_specs=[pl.BlockSpec(memory_space=pl.ANY)] * len(operands),
        out_specs=pl.BlockSpec(memory_space=pl.ANY),
        scratch_shapes=[pltpu.SemaphoreType.DMA((n, far))],
        input_output_aliases={} if out is None else {n: 0},
        compiler_params=pltpu.CompilerParams(vmem_limit_bytes=1 << 20),
        cost_estimate=pl.CostEstimate(
            flops=n * 1000000, bytes_accessed=2 * 2 * n * arrays[0].size, transcendentals=0
        ),
    )(*operands)


VMEM = pl.BlockSpec(memory_space=pltpu.VMEM)


def on_device(delta, params, momentum):
    reps = lax.axis_size("rep")
    rows, columns = params.shape[0] // reps, params.shape[1]
    groups = far_groups()
    block = jax.ShapeDtypeStruct((rows, columns), jnp.float32)
    whole = jax.ShapeDtypeStruct(params.shape, jnp.float32)
    small = pltpu.CompilerParams(vmem_limit_bytes=8 << 20)

    parts = lax.all_to_all(delta[0].reshape(reps, rows, columns), "rep", 0, 0, tiled=True)
    first_row = lax.axis_index("rep") * rows
    average, weights = pl.pallas_call(
        quarter_kernel,
        name="quarter",
        out_shape=(block, jax.ShapeDtypeStruct((len(groups[0]), rows, columns), jnp.bfloat16)),
        in_specs=[VMEM] * 3,
        out_specs=(VMEM, VMEM),
        compiler_params=small,
    )(
        parts,
        lax.dynamic_slice_in_dim(params, first_row, rows, 0),
        lax.dynamic_slice_in_dim(momentum, first_row, rows, 0),
    )

    own = lax.all_to_all(weights, PLANE, 0, 0, axis_index_groups=groups, tiled=True)
    by_x = send(own, lambda x, y, core: (beside(x, core), y, core))
    by_y = send(own, lambda x, y, core: (x, beside(y, core), core))
    by_both = send(own, lambda x, y, core: (beside(x, core), beside(y, core), core))
    average_y = send(average, lambda x, y, core: (x, y ^ 1, core))
    swap = lambda array: send(array, lambda x, y, core: (x, y, 1 - core))
    own_swap = swap(own)
    average_swap = swap(average)
    x_swap = swap(by_x)
    y_swap = swap(by_y)
    average_y_swap = swap(average_y)
    both_swap = swap(by_both)

    shape = (params.shape[0] * NX * NY // 2, columns)
    out = place(
        [(own, (0, 0, 0)), (own_swap, (0, 0, 1)), (by_x, (1, 0, 0)), (by_y, (0, 1, 0))],
        None,
        shape,
    )
    out = place(
        [(x_swap, (1, 0, 1)), (y_swap, (0, 1, 1)), (by_both, (1, 1, 0)), (both_swap, (1, 1, 1))],
        out,
        shape,
    )

    params_next, momentum_next = pl.pallas_call(
        whole_kernel,
        name="whole",
        out_shape=(whole, whole),
        in_specs=[VMEM] * 6,
        out_specs=(VMEM, VMEM),
        compiler_params=small,
        cost_estimate=pl.CostEstimate(flops=1000000, bytes_accessed=5 << 20, transcendentals=0),
    )(average, average_y, average_swap, average_y_swap, params, momentum)
    return (params_next, momentum_next, out)


def solution(mesh):
    return jax.shard_map(
        on_device,
        mesh=mesh,
        in_specs=(P("rep", "row", "col"), P("row", "col"), P("row", "col")),
        out_specs=(P("row", "col"), P("row", "col"), P(None, "col")),
        check_vma=False,
    )
```

```python
import jax
import jax.numpy as jnp
from jax import lax
from jax.experimental import pallas as pl
from jax.experimental.pallas import tpu as pltpu
from jax.sharding import PartitionSpec as P


PLANE = ("rep", "row")
NX, NY = 4, 8


def index(x, y, core):
    return ((y % NY % 2) * 2 + core) * (NX * NY // 2) + (y % NY // 2) * NX + x % NX


def beside(i, core):
    return i + 1 - 2 * ((i + core) % 2)


def send(array, partner):
    pairs = [
        (index(x, y, core), index(*partner(x, y, core)))
        for x in range(NX)
        for y in range(NY)
        for core in range(2)
    ]
    return lax.ppermute(array, PLANE, pairs)


def far_groups():
    return [
        [index(x + 2 * j, y + 2 * i, core) for i in range(NY // 2) for j in range(NX // 2)]
        for x in range(2)
        for y in range(2)
        for core in range(2)
    ]


def update(average, params, momentum):
    momentum_next = 0.9 * momentum + average
    params_next = params - 0.7 * (average + 0.9 * momentum_next)
    return (params_next, momentum_next)


def quarter_kernel(parts_ref, params_ref, momentum_ref, average_ref, weights_ref):
    reps = parts_ref.shape[0]
    total = parts_ref[0].astype(jnp.float32)
    for i in range(1, reps):
        total += parts_ref[i].astype(jnp.float32)
    average = total / reps
    average_ref[...] = average
    params_next, _ = update(average, params_ref[...], momentum_ref[...])
    for i in range(weights_ref.shape[0]):
        weights_ref[i] = params_next.astype(jnp.bfloat16)


def whole_kernel(own_ref, y_ref, core_ref, both_ref, params_ref, momentum_ref, params_out, momentum_out):
    rep = lax.axis_index("rep")
    y, core = rep // 2, lax.rem(rep, 2)
    rows = own_ref.shape[0]
    for ref, flip_y, flip_core in ((own_ref, 0, 0), (y_ref, 1, 0), (core_ref, 0, 1), (both_ref, 1, 1)):
        block = (1 - y if flip_y else y) * 2 + (1 - core if flip_core else core)
        at = pl.ds(pl.multiple_of(block * rows, rows), rows)
        params_out[at], momentum_out[at] = update(ref[...], params_ref[at], momentum_ref[at])


def place_kernel(flips, n, *refs):
    out_ref, sems = refs[-2:]
    rep, row = lax.axis_index("rep"), lax.axis_index("row")
    x, y, core = lax.rem(row, 2), rep // 2, lax.rem(rep, 2)
    copies = []
    for i, (ref, (fx, fy, fc)) in enumerate(zip(refs[:n], flips)):
        far, rows, _ = ref.shape
        near = ((1 - x if fx else x) * 2 + (1 - y if fy else y)) * 2 + (1 - core if fc else core)
        for k in range(far):
            at = pl.multiple_of((k * 8 + near) * rows, rows)
            copy = pltpu.make_async_copy(ref.at[k], out_ref.at[pl.ds(at, rows)], sems.at[i, k])
            copy.start()
            copies.append(copy)
    for copy in copies:
        copy.wait()


def place(blocks, out, shape):
    arrays, flips = zip(*blocks)
    n = len(arrays)
    far = arrays[0].shape[0]
    kernel = lambda *refs: place_kernel(flips, n, *refs)
    operands = arrays if out is None else (*arrays, out)
    return pl.pallas_call(
        kernel,
        name="place",
        out_shape=jax.ShapeDtypeStruct(shape, jnp.bfloat16),
        in_specs=[pl.BlockSpec(memory_space=pl.ANY)] * len(operands),
        out_specs=pl.BlockSpec(memory_space=pl.ANY),
        scratch_shapes=[pltpu.SemaphoreType.DMA((n, far))],
        input_output_aliases={} if out is None else {n: 0},
        compiler_params=pltpu.CompilerParams(vmem_limit_bytes=1 << 20),
        cost_estimate=pl.CostEstimate(
            flops=n * 1000000, bytes_accessed=2 * 2 * n * arrays[0].size, transcendentals=0
        ),
    )(*operands)


VMEM = pl.BlockSpec(memory_space=pltpu.VMEM)


def on_device(delta, params, momentum):
    reps = lax.axis_size("rep")
    rows, columns = params.shape[0] // reps, params.shape[1]
    groups = far_groups()
    block = jax.ShapeDtypeStruct((rows, columns), jnp.float32)
    whole = jax.ShapeDtypeStruct(params.shape, jnp.float32)
    small = pltpu.CompilerParams(vmem_limit_bytes=8 << 20)

    parts = lax.all_to_all(delta[0].reshape(reps, rows, columns), "rep", 0, 0, tiled=True)
    first_row = lax.axis_index("rep") * rows
    average, weights = pl.pallas_call(
        quarter_kernel,
        name="quarter",
        out_shape=(block, jax.ShapeDtypeStruct((len(groups[0]), rows, columns), jnp.bfloat16)),
        in_specs=[VMEM] * 3,
        out_specs=(VMEM, VMEM),
        compiler_params=small,
    )(
        parts,
        lax.dynamic_slice_in_dim(params, first_row, rows, 0),
        lax.dynamic_slice_in_dim(momentum, first_row, rows, 0),
    )

    own = lax.all_to_all(weights, PLANE, 0, 0, axis_index_groups=groups, tiled=True)
    by_x = send(own, lambda x, y, core: (beside(x, core), y, core))
    by_y = send(own, lambda x, y, core: (x, beside(y, core), core))
    by_both = send(own, lambda x, y, core: (beside(x, core), beside(y, core), core))
    average_y = send(average, lambda x, y, core: (x, y ^ 1, core))
    swap = lambda array: send(array, lambda x, y, core: (x, y, 1 - core))
    own_swap = swap(own)
    average_swap = swap(average)
    x_swap = swap(by_x)
    y_swap = swap(by_y)
    average_y_swap = swap(average_y)
    both_swap = swap(by_both)

    shape = (params.shape[0] * NX * NY // 2, columns)
    out = place(
        [
            (own, (0, 0, 0)),
            (own_swap, (0, 0, 1)),
            (by_x, (1, 0, 0)),
            (x_swap, (1, 0, 1)),
            (by_y, (0, 1, 0)),
            (y_swap, (0, 1, 1)),
        ],
        None,
        shape,
    )
    out = place([(by_both, (1, 1, 0))], out, shape)
    out = place([(both_swap, (1, 1, 1))], out, shape)

    params_next, momentum_next = pl.pallas_call(
        whole_kernel,
        name="whole",
        out_shape=(whole, whole),
        in_specs=[VMEM] * 6,
        out_specs=(VMEM, VMEM),
        compiler_params=small,
        cost_estimate=pl.CostEstimate(flops=1000000, bytes_accessed=5 << 20, transcendentals=0),
    )(average, average_y, average_swap, average_y_swap, params, momentum)
    return (params_next, momentum_next, out)


def solution(mesh):
    return jax.shard_map(
        on_device,
        mesh=mesh,
        in_specs=(P("rep", "row", "col"), P("row", "col"), P("row", "col")),
        out_specs=(P("row", "col"), P("row", "col"), P(None, "col")),
        check_vma=False,
    )
```

```python
import jax
import jax.numpy as jnp
from jax import lax
from jax.experimental import pallas as pl
from jax.experimental.pallas import tpu as pltpu
from jax.sharding import PartitionSpec as P


PLANE = ("rep", "row")
NX, NY = 4, 8


def index(x, y, core):
    return ((y % NY % 2) * 2 + core) * (NX * NY // 2) + (y % NY // 2) * NX + x % NX


def beside(i, core):
    return i + 1 - 2 * ((i + core) % 2)


def send(array, partner):
    pairs = [
        (index(x, y, core), index(*partner(x, y, core)))
        for x in range(NX)
        for y in range(NY)
        for core in range(2)
    ]
    return lax.ppermute(array, PLANE, pairs)


def far_groups():
    return [
        [index(x + 2 * j, y + 2 * i, core) for i in range(NY // 2) for j in range(NX // 2)]
        for x in range(2)
        for y in range(2)
        for core in range(2)
    ]


def update(average, params, momentum):
    momentum_next = 0.9 * momentum + average
    params_next = params - 0.7 * (average + 0.9 * momentum_next)
    return (params_next, momentum_next)


VMEM = pl.BlockSpec(memory_space=pltpu.VMEM)
ANY = pl.BlockSpec(memory_space=pl.ANY)
SMALL = pltpu.CompilerParams(vmem_limit_bytes=8 << 20)


def fetch_kernel(a_ref, b_ref, a_out, b_out, sems):
    copies = [
        pltpu.make_async_copy(a_ref, a_out, sems.at[0]),
        pltpu.make_async_copy(b_ref, b_out, sems.at[1]),
    ]
    for copy in copies:
        copy.start()
    for copy in copies:
        copy.wait()


def fetch(a, b):
    return pl.pallas_call(
        fetch_kernel,
        name="fetch",
        out_shape=(jax.ShapeDtypeStruct(a.shape, a.dtype), jax.ShapeDtypeStruct(b.shape, b.dtype)),
        in_specs=[pl.BlockSpec(memory_space=pltpu.HBM)] * 2,
        out_specs=(VMEM, VMEM),
        scratch_shapes=[pltpu.SemaphoreType.DMA((2,))],
        compiler_params=SMALL,
        cost_estimate=pl.CostEstimate(flops=1000000, bytes_accessed=4 << 20, transcendentals=0),
    )(a, b)


def quarter_kernel(parts_ref, params_ref, momentum_ref, average_ref, weights_ref):
    reps, rows, _ = parts_ref.shape
    at = pl.ds(pl.multiple_of(lax.axis_index("rep") * rows, rows), rows)
    total = parts_ref[0].astype(jnp.float32)
    for i in range(1, reps):
        total += parts_ref[i].astype(jnp.float32)
    average = total / reps
    average_ref[...] = average
    params_next, _ = update(average, params_ref[at], momentum_ref[at])
    for i in range(weights_ref.shape[0]):
        weights_ref[i] = params_next.astype(jnp.bfloat16)


def join_kernel(*refs):
    out_ref, start = refs[-1], 0
    for ref in refs[:-1]:
        out_ref[start : start + ref.shape[0]] = ref[...]
        start += ref.shape[0]


def join(*arrays):
    n = sum(array.shape[0] for array in arrays)
    return pl.pallas_call(
        join_kernel,
        name="join",
        out_shape=jax.ShapeDtypeStruct((n, *arrays[0].shape[1:]), arrays[0].dtype),
        in_specs=[VMEM] * len(arrays),
        out_specs=VMEM,
        compiler_params=SMALL,
    )(*arrays)


def whole_kernel(own_ref, y_ref, swap_ref, params_ref, momentum_ref, params_out, momentum_out):
    rep = lax.axis_index("rep")
    y, core = rep // 2, lax.rem(rep, 2)
    rows = own_ref.shape[0]
    blocks = (
        (y * 2 + core, own_ref[...]),
        ((1 - y) * 2 + core, y_ref[...]),
        (y * 2 + 1 - core, swap_ref[:rows]),
        ((1 - y) * 2 + 1 - core, swap_ref[rows:]),
    )
    for block, average in blocks:
        at = pl.ds(pl.multiple_of(block * rows, rows), rows)
        params_out[at], momentum_out[at] = update(average, params_ref[at], momentum_ref[at])


def place_kernel(spots, *refs):
    out_ref, sems = refs[-2:]
    rep, row = lax.axis_index("rep"), lax.axis_index("row")
    x, y, core = lax.rem(row, 2), rep // 2, lax.rem(rep, 2)
    copies = []
    for ref, spot in zip(refs, spots):
        for i, (k, fx, fy, fc) in enumerate(spot):
            rows = ref.shape[1]
            near = ((1 - x if fx else x) * 2 + (1 - y if fy else y)) * 2 + (1 - core if fc else core)
            at = pl.multiple_of((k * 8 + near) * rows, rows)
            copy = pltpu.make_async_copy(ref.at[i], out_ref.at[pl.ds(at, rows)], sems.at[len(copies)])
            copy.start()
            copies.append(copy)
    for copy in copies:
        copy.wait()


def place(blocks, out, shape):
    arrays, spots = zip(*blocks)
    operands = arrays if out is None else (*arrays, out)
    size = sum(array.size for array in arrays)
    return pl.pallas_call(
        lambda *refs: place_kernel(spots, *refs),
        name="place",
        out_shape=jax.ShapeDtypeStruct(shape, jnp.bfloat16),
        in_specs=[ANY] * len(operands),
        out_specs=ANY,
        scratch_shapes=[pltpu.SemaphoreType.DMA((sum(map(len, spots)),))],
        input_output_aliases={} if out is None else {len(arrays): 0},
        compiler_params=pltpu.CompilerParams(vmem_limit_bytes=1 << 20),
        cost_estimate=pl.CostEstimate(flops=1000000, bytes_accessed=4 * size, transcendentals=0),
    )(*operands)


def on_device(delta, params, momentum):
    reps = lax.axis_size("rep")
    rows, columns = params.shape[0] // reps, params.shape[1]
    groups = far_groups()
    far = len(groups[0])
    block = jax.ShapeDtypeStruct((rows, columns), jnp.float32)
    whole = jax.ShapeDtypeStruct(params.shape, jnp.float32)

    parts = lax.all_to_all(delta[0].reshape(reps, rows, columns), "rep", 0, 0, tiled=True)
    params, momentum = fetch(params, momentum)
    average, weights = pl.pallas_call(
        quarter_kernel,
        name="quarter",
        out_shape=(block, jax.ShapeDtypeStruct((far, rows, columns), jnp.bfloat16)),
        in_specs=[VMEM] * 3,
        out_specs=(VMEM, VMEM),
        compiler_params=SMALL,
    )(parts, params, momentum)

    own = lax.all_to_all(weights, PLANE, 0, 0, axis_index_groups=groups, tiled=True)
    diagonal = lambda x, y, core: (beside(x, core), beside(y, core), core)
    other_core = lambda x, y, core: (x, y, 1 - core)
    by_x = send(own, lambda x, y, core: (beside(x, core), y, core))
    by_y = send(own, lambda x, y, core: (x, beside(y, core), core))
    average_y = send(average, lambda x, y, core: (x, y ^ 1, core))
    both_0 = send(own[: far // 2], diagonal)
    both_1 = send(own[far // 2 :], diagonal)
    average_swap = send(join(average, average_y), other_core)
    near_swap = send(join(own, by_x, by_y), other_core)
    swap_0 = send(both_0, other_core)
    swap_1 = send(both_1, other_core)

    shape = (params.shape[0] * NX * NY // 2, columns)
    spots = lambda fx, fy, fc, ks=range(far): tuple((k, fx, fy, fc) for k in ks)
    first, second = range(far // 2), range(far // 2, far)
    out = place(
        [
            (own, spots(0, 0, 0)),
            (by_x, spots(1, 0, 0)),
            (by_y, spots(0, 1, 0)),
            (near_swap, spots(0, 0, 1) + spots(1, 0, 1) + spots(0, 1, 1)),
        ],
        None,
        shape,
    )
    out = place(
        [
            (both_0, spots(1, 1, 0, first)),
            (both_1, spots(1, 1, 0, second)),
            (swap_0, spots(1, 1, 1, first)),
        ],
        out,
        shape,
    )
    out = place([(swap_1, spots(1, 1, 1, second))], out, shape)

    params_next, momentum_next = pl.pallas_call(
        whole_kernel,
        name="whole",
        out_shape=(whole, whole),
        in_specs=[VMEM] * 5,
        out_specs=(VMEM, VMEM),
        compiler_params=SMALL,
        cost_estimate=pl.CostEstimate(flops=1000000, bytes_accessed=5 << 20, transcendentals=0),
    )(average, average_y, average_swap, params, momentum)
    return (params_next, momentum_next, out)


def solution(mesh):
    return jax.shard_map(
        on_device,
        mesh=mesh,
        in_specs=(P("rep", "row", "col"), P("row", "col"), P("row", "col")),
        out_specs=(P("row", "col"), P("row", "col"), P(None, "col")),
        check_vma=False,
    )
```

```python
import jax
import jax.numpy as jnp
from jax import lax
from jax.experimental import pallas as pl
from jax.experimental.pallas import tpu as pltpu
from jax.sharding import PartitionSpec as P


PLANE = ("rep", "row")
NX, NY = 4, 8


def index(x, y, core):
    return ((y % NY % 2) * 2 + core) * (NX * NY // 2) + (y % NY // 2) * NX + x % NX


def beside(i, core):
    return i + 1 - 2 * ((i + core) % 2)


def send(array, partner):
    pairs = [
        (index(x, y, core), index(*partner(x, y, core)))
        for x in range(NX)
        for y in range(NY)
        for core in range(2)
    ]
    return lax.ppermute(array, PLANE, pairs)


def far_groups():
    return [
        [index(x + 2 * j, y + 2 * i, core) for i in range(NY // 2) for j in range(NX // 2)]
        for x in range(2)
        for y in range(2)
        for core in range(2)
    ]


def update(average, params, momentum):
    momentum_next = 0.9 * momentum + average
    params_next = params - 0.7 * (average + 0.9 * momentum_next)
    return (params_next, momentum_next)


VMEM = pl.BlockSpec(memory_space=pltpu.VMEM)
ANY = pl.BlockSpec(memory_space=pl.ANY)
SMALL = pltpu.CompilerParams(vmem_limit_bytes=8 << 20)


def fetch_kernel(a_ref, b_ref, a_out, b_out):
    a_out[...] = a_ref[...]
    b_out[...] = b_ref[...]


def fetch(a, b):
    return pl.pallas_call(
        fetch_kernel,
        name="fetch",
        out_shape=(jax.ShapeDtypeStruct(a.shape, a.dtype), jax.ShapeDtypeStruct(b.shape, b.dtype)),
        in_specs=[VMEM] * 2,
        out_specs=(VMEM, VMEM),
        compiler_params=SMALL,
        cost_estimate=pl.CostEstimate(flops=1000000, bytes_accessed=4 << 20, transcendentals=0),
    )(a, b)


def quarter_kernel(parts_ref, params_ref, momentum_ref, average_ref, weights_ref):
    reps, rows, _ = parts_ref.shape
    at = pl.ds(pl.multiple_of(lax.axis_index("rep") * rows, rows), rows)
    total = parts_ref[0].astype(jnp.float32)
    for i in range(1, reps):
        total += parts_ref[i].astype(jnp.float32)
    average = total / reps
    average_ref[...] = average
    params_next, _ = update(average, params_ref[at], momentum_ref[at])
    for i in range(weights_ref.shape[0]):
        weights_ref[i] = params_next.astype(jnp.bfloat16)


def join_kernel(*refs):
    out_ref, start = refs[-1], 0
    for ref in refs[:-1]:
        out_ref[start : start + ref.shape[0]] = ref[...]
        start += ref.shape[0]


def join(*arrays):
    n = sum(array.shape[0] for array in arrays)
    return pl.pallas_call(
        join_kernel,
        name="join",
        out_shape=jax.ShapeDtypeStruct((n, *arrays[0].shape[1:]), arrays[0].dtype),
        in_specs=[VMEM] * len(arrays),
        out_specs=VMEM,
        compiler_params=SMALL,
    )(*arrays)


def whole_kernel(own_ref, y_ref, swap_ref, params_ref, momentum_ref, params_out, momentum_out):
    rep = lax.axis_index("rep")
    y, core = rep // 2, lax.rem(rep, 2)
    rows = own_ref.shape[0]
    blocks = (
        (y * 2 + core, own_ref[...]),
        ((1 - y) * 2 + core, y_ref[...]),
        (y * 2 + 1 - core, swap_ref[:rows]),
        ((1 - y) * 2 + 1 - core, swap_ref[rows:]),
    )
    for block, average in blocks:
        at = pl.ds(pl.multiple_of(block * rows, rows), rows)
        params_out[at], momentum_out[at] = update(average, params_ref[at], momentum_ref[at])


def place_kernel(spots, *refs):
    out_ref, sems = refs[-2:]
    rep, row = lax.axis_index("rep"), lax.axis_index("row")
    x, y, core = lax.rem(row, 2), rep // 2, lax.rem(rep, 2)
    copies = []
    for ref, spot in zip(refs, spots):
        for i, (k, fx, fy, fc) in enumerate(spot):
            rows = ref.shape[1]
            near = ((1 - x if fx else x) * 2 + (1 - y if fy else y)) * 2 + (1 - core if fc else core)
            at = pl.multiple_of((k * 8 + near) * rows, rows)
            copy = pltpu.make_async_copy(ref.at[i], out_ref.at[pl.ds(at, rows)], sems.at[len(copies)])
            copy.start()
            copies.append(copy)
    for copy in copies:
        copy.wait()


def place(blocks, out, shape):
    arrays, spots = zip(*blocks)
    operands = arrays if out is None else (*arrays, out)
    size = sum(array.size for array in arrays)
    return pl.pallas_call(
        lambda *refs: place_kernel(spots, *refs),
        name="place",
        out_shape=jax.ShapeDtypeStruct(shape, jnp.bfloat16),
        in_specs=[ANY] * len(operands),
        out_specs=ANY,
        scratch_shapes=[pltpu.SemaphoreType.DMA((sum(map(len, spots)),))],
        input_output_aliases={} if out is None else {len(arrays): 0},
        compiler_params=pltpu.CompilerParams(vmem_limit_bytes=1 << 20),
        cost_estimate=pl.CostEstimate(flops=1000000, bytes_accessed=4 * size, transcendentals=0),
    )(*operands)


def on_device(delta, params, momentum):
    reps = lax.axis_size("rep")
    rows, columns = params.shape[0] // reps, params.shape[1]
    groups = far_groups()
    far = len(groups[0])
    block = jax.ShapeDtypeStruct((rows, columns), jnp.float32)
    whole = jax.ShapeDtypeStruct(params.shape, jnp.float32)

    parts = lax.all_to_all(delta[0].reshape(reps, rows, columns), "rep", 0, 0, tiled=True)
    params, momentum = fetch(params, momentum)
    average, weights = pl.pallas_call(
        quarter_kernel,
        name="quarter",
        out_shape=(block, jax.ShapeDtypeStruct((far, rows, columns), jnp.bfloat16)),
        in_specs=[VMEM] * 3,
        out_specs=(VMEM, VMEM),
        compiler_params=SMALL,
    )(parts, params, momentum)

    own = lax.all_to_all(weights, PLANE, 0, 0, axis_index_groups=groups, tiled=True)
    diagonal = lambda x, y, core: (beside(x, core), beside(y, core), core)
    other_core = lambda x, y, core: (x, y, 1 - core)
    by_x = send(own, lambda x, y, core: (beside(x, core), y, core))
    by_y = send(own, lambda x, y, core: (x, beside(y, core), core))
    average_y = send(average, lambda x, y, core: (x, y ^ 1, core))
    both_0 = send(own[: far // 2], diagonal)
    both_1 = send(own[far // 2 :], diagonal)
    average_swap = send(join(average, average_y), other_core)
    near_swap = send(join(own, by_x, by_y), other_core)
    swap_0 = send(both_0, other_core)
    swap_1 = send(both_1, other_core)

    shape = (params.shape[0] * NX * NY // 2, columns)
    spots = lambda fx, fy, fc, ks=range(far): tuple((k, fx, fy, fc) for k in ks)
    first, second = range(far // 2), range(far // 2, far)
    out = place(
        [(own, spots(0, 0, 0)), (by_x, spots(1, 0, 0)), (by_y, spots(0, 1, 0))], None, shape
    )
    swapped = spots(0, 0, 1) + spots(1, 0, 1) + spots(0, 1, 1)
    out = place([(near_swap, swapped), (both_0, spots(1, 1, 0, first))], out, shape)
    out = place([(both_1, spots(1, 1, 0, second)), (swap_0, spots(1, 1, 1, first))], out, shape)
    out = place([(swap_1, spots(1, 1, 1, second))], out, shape)

    params_next, momentum_next = pl.pallas_call(
        whole_kernel,
        name="whole",
        out_shape=(whole, whole),
        in_specs=[VMEM] * 5,
        out_specs=(VMEM, VMEM),
        compiler_params=SMALL,
        cost_estimate=pl.CostEstimate(flops=1000000, bytes_accessed=5 << 20, transcendentals=0),
    )(average, average_y, average_swap, params, momentum)
    return (params_next, momentum_next, out)


def solution(mesh):
    return jax.shard_map(
        on_device,
        mesh=mesh,
        in_specs=(P("rep", "row", "col"), P("row", "col"), P("row", "col")),
        out_specs=(P("row", "col"), P("row", "col"), P(None, "col")),
        check_vma=False,
    )
```

```python
import jax
import jax.numpy as jnp
from jax import lax
from jax.experimental import pallas as pl
from jax.experimental.pallas import tpu as pltpu
from jax.sharding import PartitionSpec as P


PLANE = ("rep", "row")
NX, NY = 4, 8


def index(x, y, core):
    return ((y % NY % 2) * 2 + core) * (NX * NY // 2) + (y % NY // 2) * NX + x % NX


def beside(i, core):
    return i + 1 - 2 * ((i + core) % 2)


def send(array, partner):
    pairs = [
        (index(x, y, core), index(*partner(x, y, core)))
        for x in range(NX)
        for y in range(NY)
        for core in range(2)
    ]
    return lax.ppermute(array, PLANE, pairs)


def far_groups():
    return [
        [index(x + 2 * j, y + 2 * i, core) for i in range(NY // 2) for j in range(NX // 2)]
        for x in range(2)
        for y in range(2)
        for core in range(2)
    ]


def update(average, params, momentum):
    momentum_next = 0.9 * momentum + average
    params_next = params - 0.7 * (average + 0.9 * momentum_next)
    return (params_next, momentum_next)


VMEM = pl.BlockSpec(memory_space=pltpu.VMEM)
ANY = pl.BlockSpec(memory_space=pl.ANY)
SMALL = pltpu.CompilerParams(vmem_limit_bytes=8 << 20)


def fetch_kernel(a_ref, b_ref, a_out, b_out):
    a_out[...] = a_ref[...]
    b_out[...] = b_ref[...]


def fetch(a, b):
    return pl.pallas_call(
        fetch_kernel,
        name="fetch",
        out_shape=(jax.ShapeDtypeStruct(a.shape, a.dtype), jax.ShapeDtypeStruct(b.shape, b.dtype)),
        in_specs=[VMEM] * 2,
        out_specs=(VMEM, VMEM),
        compiler_params=SMALL,
        cost_estimate=pl.CostEstimate(flops=1000000, bytes_accessed=4 << 20, transcendentals=0),
    )(a, b)


def quarter_kernel(parts_ref, params_ref, momentum_ref, average_ref, weights_ref):
    reps, rows, _ = parts_ref.shape
    at = pl.ds(pl.multiple_of(lax.axis_index("rep") * rows, rows), rows)
    total = parts_ref[0].astype(jnp.float32)
    for i in range(1, reps):
        total += parts_ref[i].astype(jnp.float32)
    average = total / reps
    average_ref[...] = average
    params_next, _ = update(average, params_ref[at], momentum_ref[at])
    for i in range(weights_ref.shape[0]):
        weights_ref[i] = params_next.astype(jnp.bfloat16)


def join_kernel(*refs):
    out_ref, start = refs[-1], 0
    for ref in refs[:-1]:
        out_ref[start : start + ref.shape[0]] = ref[...]
        start += ref.shape[0]


def join(*arrays):
    n = sum(array.shape[0] for array in arrays)
    return pl.pallas_call(
        join_kernel,
        name="join",
        out_shape=jax.ShapeDtypeStruct((n, *arrays[0].shape[1:]), arrays[0].dtype),
        in_specs=[VMEM] * len(arrays),
        out_specs=VMEM,
        compiler_params=SMALL,
    )(*arrays)


def whole_kernel(own_ref, y_ref, swap_ref, params_ref, momentum_ref, params_out, momentum_out):
    rep = lax.axis_index("rep")
    y, core = rep // 2, lax.rem(rep, 2)
    rows = own_ref.shape[0]
    blocks = (
        (y * 2 + core, own_ref[...]),
        ((1 - y) * 2 + core, y_ref[...]),
        (y * 2 + 1 - core, swap_ref[:rows]),
        ((1 - y) * 2 + 1 - core, swap_ref[rows:]),
    )
    for block, average in blocks:
        at = pl.ds(pl.multiple_of(block * rows, rows), rows)
        params_out[at], momentum_out[at] = update(average, params_ref[at], momentum_ref[at])


def place_kernel(spots, *refs):
    out_ref, sems = refs[-2:]
    rep, row = lax.axis_index("rep"), lax.axis_index("row")
    x, y, core = lax.rem(row, 2), rep // 2, lax.rem(rep, 2)
    copies = []
    for ref, spot in zip(refs, spots):
        for i, (k, fx, fy, fc) in enumerate(spot):
            rows = ref.shape[1]
            near = ((1 - x if fx else x) * 2 + (1 - y if fy else y)) * 2 + (1 - core if fc else core)
            at = pl.multiple_of((k * 8 + near) * rows, rows)
            copy = pltpu.make_async_copy(ref.at[i], out_ref.at[pl.ds(at, rows)], sems.at[len(copies)])
            copy.start()
            copies.append(copy)
    for copy in copies:
        copy.wait()


def place(blocks, out, shape):
    arrays, spots = zip(*blocks)
    operands = arrays if out is None else (*arrays, out)
    size = sum(array.size for array in arrays)
    return pl.pallas_call(
        lambda *refs: place_kernel(spots, *refs),
        name="place",
        out_shape=jax.ShapeDtypeStruct(shape, jnp.bfloat16),
        in_specs=[ANY] * len(operands),
        out_specs=ANY,
        scratch_shapes=[pltpu.SemaphoreType.DMA((sum(map(len, spots)),))],
        input_output_aliases={} if out is None else {len(arrays): 0},
        compiler_params=pltpu.CompilerParams(vmem_limit_bytes=1 << 20),
        cost_estimate=pl.CostEstimate(flops=1000000, bytes_accessed=4 * size, transcendentals=0),
    )(*operands)


def on_device(delta, params, momentum):
    reps = lax.axis_size("rep")
    rows, columns = params.shape[0] // reps, params.shape[1]
    groups = far_groups()
    far = len(groups[0])
    cut = far * 3 // 4
    block = jax.ShapeDtypeStruct((rows, columns), jnp.float32)
    whole = jax.ShapeDtypeStruct(params.shape, jnp.float32)

    parts = lax.all_to_all(delta[0].reshape(reps, rows, columns), "rep", 0, 0, tiled=True)
    params, momentum = fetch(params, momentum)
    average, weights = pl.pallas_call(
        quarter_kernel,
        name="quarter",
        out_shape=(block, jax.ShapeDtypeStruct((far, rows, columns), jnp.bfloat16)),
        in_specs=[VMEM] * 3,
        out_specs=(VMEM, VMEM),
        compiler_params=SMALL,
    )(parts, params, momentum)

    own = lax.all_to_all(weights, PLANE, 0, 0, axis_index_groups=groups, tiled=True)
    diagonal = lambda x, y, core: (beside(x, core), beside(y, core), core)
    other_core = lambda x, y, core: (x, y, 1 - core)
    by_x = send(own, lambda x, y, core: (beside(x, core), y, core))
    by_y = send(own, lambda x, y, core: (x, beside(y, core), core))
    average_y = send(average, lambda x, y, core: (x, y ^ 1, core))
    both_0 = send(own[:cut], diagonal)
    both_1 = send(own[cut:], diagonal)
    average_swap = send(join(average, average_y), other_core)
    near_swap = send(join(own, by_x, by_y), other_core)
    swap_0 = send(both_0, other_core)
    swap_1 = send(both_1, other_core)

    shape = (params.shape[0] * NX * NY // 2, columns)
    spots = lambda fx, fy, fc, ks=range(far): tuple((k, fx, fy, fc) for k in ks)
    first, second = range(cut), range(cut, far)
    out = place(
        [(own, spots(0, 0, 0)), (by_x, spots(1, 0, 0)), (by_y, spots(0, 1, 0))], None, shape
    )
    swapped = spots(0, 0, 1) + spots(1, 0, 1) + spots(0, 1, 1)
    out = place([(near_swap, swapped), (both_0, spots(1, 1, 0, first))], out, shape)
    out = place([(both_1, spots(1, 1, 0, second)), (swap_0, spots(1, 1, 1, first))], out, shape)
    out = place([(swap_1, spots(1, 1, 1, second))], out, shape)

    params_next, momentum_next = pl.pallas_call(
        whole_kernel,
        name="whole",
        out_shape=(whole, whole),
        in_specs=[VMEM] * 5,
        out_specs=(VMEM, VMEM),
        compiler_params=SMALL,
        cost_estimate=pl.CostEstimate(flops=1000000, bytes_accessed=5 << 20, transcendentals=0),
    )(average, average_y, average_swap, params, momentum)
    return (params_next, momentum_next, out)


def solution(mesh):
    return jax.shard_map(
        on_device,
        mesh=mesh,
        in_specs=(P("rep", "row", "col"), P("row", "col"), P("row", "col")),
        out_specs=(P("row", "col"), P("row", "col"), P(None, "col")),
        check_vma=False,
    )
```

```python
import jax
import jax.numpy as jnp
from jax import lax
from jax.experimental import pallas as pl
from jax.experimental.pallas import tpu as pltpu
from jax.sharding import PartitionSpec as P


PLANE = ("rep", "row")
NX, NY = 4, 8


def index(x, y, core):
    return ((y % NY % 2) * 2 + core) * (NX * NY // 2) + (y % NY // 2) * NX + x % NX


def beside(i, core):
    return i + 1 - 2 * ((i + core) % 2)


def send(array, partner):
    pairs = [
        (index(x, y, core), index(*partner(x, y, core)))
        for x in range(NX)
        for y in range(NY)
        for core in range(2)
    ]
    return lax.ppermute(array, PLANE, pairs)


def far_groups():
    return [
        [index(x + 2 * j, y + 2 * i, core) for i in range(NY // 2) for j in range(NX // 2)]
        for x in range(2)
        for y in range(2)
        for core in range(2)
    ]


def update(average, params, momentum):
    momentum_next = 0.9 * momentum + average
    params_next = params - 0.7 * (average + 0.9 * momentum_next)
    return (params_next, momentum_next)


VMEM = pl.BlockSpec(memory_space=pltpu.VMEM)
ANY = pl.BlockSpec(memory_space=pl.ANY)
SMALL = pltpu.CompilerParams(vmem_limit_bytes=8 << 20)


def fetch_kernel(a_ref, b_ref, a_out, b_out):
    a_out[...] = a_ref[...]
    b_out[...] = b_ref[...]


def fetch(a, b):
    return pl.pallas_call(
        fetch_kernel,
        name="fetch",
        out_shape=(jax.ShapeDtypeStruct(a.shape, a.dtype), jax.ShapeDtypeStruct(b.shape, b.dtype)),
        in_specs=[VMEM] * 2,
        out_specs=(VMEM, VMEM),
        compiler_params=SMALL,
        cost_estimate=pl.CostEstimate(flops=1000000, bytes_accessed=4 << 20, transcendentals=0),
    )(a, b)


def quarter_kernel(parts_ref, params_ref, momentum_ref, average_ref, weights_ref):
    reps, rows, _ = parts_ref.shape
    at = pl.ds(pl.multiple_of(lax.axis_index("rep") * rows, rows), rows)
    total = parts_ref[0].astype(jnp.float32)
    for i in range(1, reps):
        total += parts_ref[i].astype(jnp.float32)
    average = total / reps
    average_ref[...] = average
    params_next, _ = update(average, params_ref[at], momentum_ref[at])
    for i in range(weights_ref.shape[0]):
        weights_ref[i] = params_next.astype(jnp.bfloat16)


def join_kernel(*refs):
    out_ref, start = refs[-1], 0
    for ref in refs[:-1]:
        out_ref[start : start + ref.shape[0]] = ref[...]
        start += ref.shape[0]


def join(*arrays):
    n = sum(array.shape[0] for array in arrays)
    return pl.pallas_call(
        join_kernel,
        name="join",
        out_shape=jax.ShapeDtypeStruct((n, *arrays[0].shape[1:]), arrays[0].dtype),
        in_specs=[VMEM] * len(arrays),
        out_specs=VMEM,
        compiler_params=SMALL,
    )(*arrays)


def whole_kernel(own_ref, y_ref, swap_ref, params_ref, momentum_ref, params_out, momentum_out):
    rep = lax.axis_index("rep")
    y, core = rep // 2, lax.rem(rep, 2)
    rows = own_ref.shape[0]
    blocks = (
        (y * 2 + core, own_ref[...]),
        ((1 - y) * 2 + core, y_ref[...]),
        (y * 2 + 1 - core, swap_ref[:rows]),
        ((1 - y) * 2 + 1 - core, swap_ref[rows:]),
    )
    for block, average in blocks:
        at = pl.ds(pl.multiple_of(block * rows, rows), rows)
        params_out[at], momentum_out[at] = update(average, params_ref[at], momentum_ref[at])


def place_kernel(spots, *refs):
    out_ref, sems = refs[-2:]
    rep, row = lax.axis_index("rep"), lax.axis_index("row")
    x, y, core = lax.rem(row, 2), rep // 2, lax.rem(rep, 2)
    copies = []
    for ref, spot in zip(refs, spots):
        for i, (k, fx, fy, fc) in enumerate(spot):
            rows = ref.shape[1]
            near = ((1 - x if fx else x) * 2 + (1 - y if fy else y)) * 2 + (1 - core if fc else core)
            at = pl.multiple_of((k * 8 + near) * rows, rows)
            copy = pltpu.make_async_copy(ref.at[i], out_ref.at[pl.ds(at, rows)], sems.at[len(copies)])
            copy.start()
            copies.append(copy)
    for copy in copies:
        copy.wait()


def place(blocks, out, shape):
    arrays, spots = zip(*blocks)
    operands = arrays if out is None else (*arrays, out)
    size = sum(array.size for array in arrays)
    return pl.pallas_call(
        lambda *refs: place_kernel(spots, *refs),
        name="place",
        out_shape=jax.ShapeDtypeStruct(shape, jnp.bfloat16),
        in_specs=[ANY] * len(operands),
        out_specs=ANY,
        scratch_shapes=[pltpu.SemaphoreType.DMA((sum(map(len, spots)),))],
        input_output_aliases={} if out is None else {len(arrays): 0},
        compiler_params=pltpu.CompilerParams(vmem_limit_bytes=1 << 20),
        cost_estimate=pl.CostEstimate(flops=1000000, bytes_accessed=4 * size, transcendentals=0),
    )(*operands)


def on_device(delta, params, momentum):
    reps = lax.axis_size("rep")
    rows, columns = params.shape[0] // reps, params.shape[1]
    groups = far_groups()
    far = len(groups[0])
    block = jax.ShapeDtypeStruct((rows, columns), jnp.float32)
    whole = jax.ShapeDtypeStruct(params.shape, jnp.float32)

    parts = lax.all_to_all(delta[0].reshape(reps, rows, columns), "rep", 0, 0, tiled=True)
    params, momentum = fetch(params, momentum)
    average, weights = pl.pallas_call(
        quarter_kernel,
        name="quarter",
        out_shape=(block, jax.ShapeDtypeStruct((far, rows, columns), jnp.bfloat16)),
        in_specs=[VMEM] * 3,
        out_specs=(VMEM, VMEM),
        compiler_params=SMALL,
    )(parts, params, momentum)

    own = lax.all_to_all(weights, PLANE, 0, 0, axis_index_groups=groups, tiled=True)
    diagonal = lambda x, y, core: (beside(x, core), beside(y, core), core)
    other_core = lambda x, y, core: (x, y, 1 - core)
    by_x = send(own, lambda x, y, core: (beside(x, core), y, core))
    by_y = send(own, lambda x, y, core: (x, beside(y, core), core))
    average_y = send(average, lambda x, y, core: (x, y ^ 1, core))
    both = send(own, diagonal)
    average_swap = send(join(average, average_y), other_core)
    near_swap = send(join(own, by_x, by_y), other_core)
    both_swap = send(both, other_core)

    shape = (params.shape[0] * NX * NY // 2, columns)
    spots = lambda fx, fy, fc: tuple((k, fx, fy, fc) for k in range(far))
    out = place(
        [(own, spots(0, 0, 0)), (by_x, spots(1, 0, 0)), (by_y, spots(0, 1, 0))], None, shape
    )
    swapped = spots(0, 0, 1) + spots(1, 0, 1) + spots(0, 1, 1)
    out = place([(near_swap, swapped)], out, shape)
    out = place([(both, spots(1, 1, 0))], out, shape)
    out = place([(both_swap, spots(1, 1, 1))], out, shape)

    params_next, momentum_next = pl.pallas_call(
        whole_kernel,
        name="whole",
        out_shape=(whole, whole),
        in_specs=[VMEM] * 5,
        out_specs=(VMEM, VMEM),
        compiler_params=SMALL,
        cost_estimate=pl.CostEstimate(flops=1000000, bytes_accessed=5 << 20, transcendentals=0),
    )(average, average_y, average_swap, params, momentum)
    return (params_next, momentum_next, out)


def solution(mesh):
    return jax.shard_map(
        on_device,
        mesh=mesh,
        in_specs=(P("rep", "row", "col"), P("row", "col"), P("row", "col")),
        out_specs=(P("row", "col"), P("row", "col"), P(None, "col")),
        check_vma=False,
    )
```
